32 devices in a mesh: dp: 2 (over x), expert: 4 (over z), mp: 4 (over y, core).
Axes of the slice: x: 2, y: 2, z: 4, core: 2. Of those that a mesh axis runs over, the one named last changes fastest.
Arguments:
- tokens: bfloat16 [512, 4096], P('dp', ('expert', 'mp')), may hold values from -6 to 6
- expert_index: int32 [512, 2], P('dp'), may hold values from 0 to 3, as said below
- slot_index: int32 [512, 2], P('dp'), may hold values from 0 to 191, as said below
- norm_gain: float32 [4096], P(('expert', 'mp')), may hold values from 0.1 to 1.9
- router_weight: bfloat16 [4, 4096], P(None, ('expert', 'mp')), may hold values from -8 to 8
- gate_weight: bfloat16 [4, 7168, 4096], P('expert', ('dp', 'mp')), may hold values from -0.09375 to 0.09375
- up_weight: bfloat16 [4, 7168, 4096], P('expert', ('dp', 'mp')), may hold values from -0.09375 to 0.09375
- down_weight: bfloat16 [4, 7168, 4096], P('expert', ('dp', 'mp')), may hold values from -0.09375 to 0.09375
- final_gain: float32 [4096], replicated, may hold values from 0.1 to 1.9
- head_weight: bfloat16 [16384, 4096], P(('expert', 'mp')), may hold values from -8 to 8
Outputs:
- layer_out: bfloat16 [512, 4096], P('dp', ('expert', 'mp'))
- head_logsum: float32 [512], P('dp')
- router_penalty: float32 [], replicated
- head_penalty: float32 [], replicated
The draws below stay inside these ranges and needn't reach their ends.
Inputs may be any that keep to these rules, and one draw needn't show every extreme that they name: `expert_index`: each row names 2 different experts. In each aligned block of 256 rows every expert is named at least once and at most 192 times; in every block two experts are named exactly 192 times, and one of them is the same expert in all blocks. `slot_index`: within each aligned block of 256 rows, the choices that name one expert hold the slots 0, 1, 2, ... in the order of rows, and within a row in the order of choices.
All inputs are finite; a program needn't handle non-finite values.
Results may differ from the reference program's by a relative error of at most 0.01115.
Values may be sent and summed in bfloat16 or wider, within the bound.
No kernel may reach another device: no remote copies, remote signals or barrier semaphores. Data moves between devices by JAX's collectives and lax.ppermute only.
A program may use at most 128 MiB of HBM per device.

```python
import math
import jax
import jax.numpy as jnp
from jax import lax

D = 4096
FF = 7168
VOCAB = 16384
TOP = 2
TOK_DP = 256
EXPERTS = 4
TOKENS = 512
CAPACITY = 192
SLOTS = 384


def routing_tables(key):
    blocks = TOKENS // TOK_DP
    remain = 2 * TOK_DP - 2 * CAPACITY
    others = EXPERTS - 2
    base_count = remain // others
    extra_count = remain % others
    full_expert = jax.random.randint(jax.random.fold_in(key, 5), (), 0, EXPERTS)

    def one_block(block_key):
        key_order = jax.random.fold_in(block_key, 1)
        key_moved = jax.random.fold_in(block_key, 2)
        key_shuffle = jax.random.fold_in(block_key, 3)
        key_swap = jax.random.fold_in(block_key, 4)
        rest_order = 1 + jax.random.permutation(key_order, EXPERTS - 1).astype(jnp.int32)
        rank_expert = (full_expert + jnp.concatenate([jnp.zeros((1,), jnp.int32), rest_order])) % EXPERTS
        rank_ids = jnp.arange(others, dtype=jnp.int32)
        counts_rest = base_count + (rank_ids < extra_count).astype(jnp.int32)
        moved_count = jax.random.randint(key_moved, (others,), 0, base_count // 4 + 1)
        counts_rest = counts_rest - moved_count + jnp.roll(moved_count, 1)
        counts = jnp.concatenate([jnp.full((2,), CAPACITY, jnp.int32), counts_rest])
        bounds = jnp.cumsum(counts)
        places = jnp.arange(2 * TOK_DP, dtype=jnp.int32)
        rank_of = jnp.sum((places[:, None] >= bounds[None, :]).astype(jnp.int32), axis=1)
        labels = rank_expert[rank_of]
        choice_pairs = jnp.stack([labels[:TOK_DP], labels[TOK_DP:]], axis=1)
        shuffle = jax.random.permutation(key_shuffle, TOK_DP)
        choice_pairs = choice_pairs[shuffle]
        swap_order = jax.random.randint(key_swap, (TOK_DP, 1), 0, 2)
        choice_pairs = jnp.where(swap_order == 1, choice_pairs[:, ::-1], choice_pairs)
        flat_pairs = choice_pairs.reshape(-1)
        hit_table = (flat_pairs[:, None] == jnp.arange(EXPERTS, dtype=jnp.int32)[None, :]).astype(jnp.int32)
        running = jnp.cumsum(hit_table, axis=0)
        slot_table = jnp.sum(hit_table * running, axis=1) - 1
        return (choice_pairs.astype(jnp.int32), slot_table.reshape(TOK_DP, 2).astype(jnp.int32))
    block_keys = jax.random.split(jax.random.fold_in(key, 7), blocks)
    chosen, slotted = jax.vmap(one_block)(block_keys)
    return (chosen.reshape(TOKENS, 2), slotted.reshape(TOKENS, 2))


def draw_expert_index(key, part):
    return routing_tables(jax.random.fold_in(key, 11))[0]


def draw_slot_index(key, part):
    return routing_tables(jax.random.fold_in(key, 11))[1]


def drawn_rows(key, rows, width, scale):
    base_key = jax.random.fold_in(key, 1)
    values = jax.random.normal(base_key, (rows, width), jnp.float32) * scale
    return jnp.clip(values, -8.0, 8.0).astype(jnp.bfloat16)


def draw_router_weight(key, part):
    return drawn_rows(jax.random.fold_in(key, 21), EXPERTS, D, 1.0 / math.sqrt(D))


def draw_head_weight(key, part):
    return drawn_rows(jax.random.fold_in(key, 31), VOCAB, D, 3.0 / math.sqrt(D))


def with_spikes(drawn, own_key, source, target, blocks, factor):
    owner, partner = [(jnp.arange(drawn.shape[dim]) // (drawn.shape[dim] // blocks)).reshape([-1 if axis == dim else 1 for axis in range(drawn.ndim)]) for dim in (source, target)]
    chosen = jax.random.permutation(own_key, blocks)[partner]
    strong = (owner == chosen) | (owner == (partner + blocks // 2) % blocks)
    return jnp.where(strong, factor * drawn, drawn)


def steps_of(own_key, extent, pieces, least, top_value):
    level, own = 1.0, jax.random.fold_in(own_key, 6)
    for axis_at, parts in pieces:
        draws = jnp.exp(jax.random.uniform(jax.random.fold_in(own, axis_at), (parts,), jnp.float32, least / len(pieces), top_value / len(pieces)))
        level = level * jnp.repeat(draws, extent[axis_at] // parts).reshape([-1 if axis == axis_at else 1 for axis in range(len(extent))])
    return level


def noise(own_key, dims, deviation, bound, cuts=(), held_as=jnp.bfloat16):
    array = jax.random.normal(own_key, dims, jnp.float32) * deviation
    if len(cuts) > 0:
        array = steps_of(own_key, dims, cuts, -0.22, 0.18) * array
    return jnp.clip(array, min=-bound, max=bound).astype(held_as)


def noise_with(key, shape, scale, limit, shards, heavy, kind=jnp.bfloat16):
    values = scale * jax.random.normal(key, shape, jnp.float32)
    if shards:
        values = values * steps_of(key, shape, shards, -0.22, 0.18)
    return jnp.clip(with_spikes(values, jax.random.fold_in(key, 3), *heavy), -limit, limit).astype(kind)


def setup_inputs(seed: int = 0) -> dict:
    arg_keys = jax.random.split(jax.random.key(seed), 11)
    return {
        "tokens": noise(arg_keys[0], (TOKENS, D), 1.0, 6.0, ((0, 2), (1, 16))),
        "expert_index": draw_expert_index(jax.random.fold_in(arg_keys[10], 71), 0),
        "slot_index": draw_slot_index(jax.random.fold_in(arg_keys[10], 71), 0),
        "norm_gain": jnp.clip(1.0 + 0.18 * jax.random.normal(arg_keys[3], (D,), jnp.float32), 0.1, 1.9),
        "router_weight": draw_router_weight(jax.random.fold_in(arg_keys[10], 71), 0),
        "gate_weight": noise(arg_keys[5], (EXPERTS, FF, D), D ** -0.5, 0.09375, ((0, 4), (1, 8))),
        "up_weight": noise(arg_keys[6], (EXPERTS, FF, D), D ** -0.5, 0.09375, ((0, 4), (1, 8))),
        "down_weight": noise_with(arg_keys[7], (EXPERTS, FF, D), FF ** -0.5, 0.09375, ((0, 4), (1, 8)), (1, 2, 8, 2.0)),
        "final_gain": jnp.clip(1.0 + 0.18 * jax.random.normal(arg_keys[8], (D,), jnp.float32), 0.1, 1.9),
        "head_weight": draw_head_weight(jax.random.fold_in(arg_keys[10], 71), 0),
    }


epsilon = 1e-05

def run_expert(operands):
    slot_rows, gate_matrix, up_matrix, down_matrix = operands
    gate_value = jnp.dot(slot_rows, gate_matrix.T, preferred_element_type=jnp.float32)
    up_value = jnp.dot(slot_rows, up_matrix.T, preferred_element_type=jnp.float32)
    hidden = (jax.nn.silu(gate_value) * up_value).astype(jnp.bfloat16)
    return jnp.dot(hidden, down_matrix, preferred_element_type=jnp.float32).astype(jnp.bfloat16)

def reference(tokens, expert_index, slot_index, norm_gain, router_weight, gate_weight, up_weight, down_weight, final_gain, head_weight):
    tokens_float = tokens.astype(jnp.float32)
    inverse = lax.rsqrt(lax.optimization_barrier(jnp.mean(tokens_float * tokens_float, axis=1)) + epsilon)
    normed = tokens_float * inverse[:, None] * norm_gain[None, :]
    normed_rows = normed.astype(jnp.bfloat16)
    router_logits = jnp.dot(normed, router_weight.astype(jnp.float32).T, precision=lax.Precision.HIGHEST)
    router_logsum = jax.nn.logsumexp(router_logits, axis=1)
    picked = jnp.take_along_axis(router_logits, expert_index, axis=1)
    gate_weights = jax.nn.softmax(picked, axis=1)
    shard_number = jnp.arange(TOKENS, dtype=jnp.int32) // TOK_DP
    position = shard_number[:, None] * CAPACITY + slot_index
    buffer = jnp.zeros((EXPERTS, SLOTS, D), jnp.bfloat16)
    buffer = buffer.at[expert_index.reshape(-1), position.reshape(-1)].set(jnp.repeat(normed_rows, TOP, axis=0))
    outputs = lax.map(run_expert, (buffer, gate_weight, up_weight, down_weight))
    picked_rows = outputs[expert_index, position]
    combined = lax.optimization_barrier(jnp.sum(gate_weights[:, :, None] * picked_rows.astype(jnp.float32), axis=1))
    layer_out = (tokens_float + combined).astype(jnp.bfloat16)
    layer_float = layer_out.astype(jnp.float32)
    head_scale = lax.rsqrt(lax.optimization_barrier(jnp.mean(layer_float * layer_float, axis=1)) + epsilon)
    head_in = (layer_float * head_scale[:, None] * final_gain[None, :]).astype(jnp.bfloat16)
    logits = jnp.dot(head_in, head_weight.T, preferred_element_type=jnp.float32)
    head_logsum = jax.nn.logsumexp(logits, axis=1)
    return (layer_out, head_logsum, jnp.mean(router_logsum * router_logsum), jnp.mean(head_logsum * head_logsum))
```

```python
import jax
import jax.numpy as jnp
from jax import lax
from jax.sharding import PartitionSpec as P

epsilon = 1e-05
GAIN_ROWS = 16


def axis_bits(axis):
    size = lax.axis_size(axis)
    bits = []
    bit = 1
    while bit < size:
        bits.append(bit)
        bit *= 2
    return bits


def swap(value, axis, mask):
    size = lax.axis_size(axis)
    return lax.ppermute(value, axis, [(i, i ^ mask) for i in range(size)])


def upper(axis, bit):
    return (lax.axis_index(axis) & bit) != 0


def doubling(value, stages):
    for axis, bit in stages:
        other = swap(value, axis, bit)
        high = upper(axis, bit)
        value = jnp.stack([jnp.where(high, other, value), jnp.where(high, value, other)])
    return value


def piece_of(value, stages, place):
    index = tuple(1 if place[axis] & bit else 0 for axis, bit in reversed(stages))
    return value[index]


def halving(value, dims, stages):
    dims = list(dims)
    for axis, bit in stages:
        at = dims.index((axis, bit))
        low = lax.index_in_dim(value, 0, at, keepdims=False)
        top = lax.index_in_dim(value, 1, at, keepdims=False)
        high = upper(axis, bit)
        arrived = swap(jnp.where(high, low, top), axis, bit)
        kept = jnp.where(high, top, low)
        value = (kept.astype(jnp.float32) + arrived.astype(jnp.float32)).astype(value.dtype)
        dims.pop(at)
    return value


def gather_direct(value, axis):
    size = lax.axis_size(axis)
    blocks = [value] + [swap(value, axis, mask) for mask in range(1, size)]
    for bit in axis_bits(axis):
        high = upper(axis, bit)
        blocks = [jnp.where(high, blocks[k ^ bit], blocks[k]) for k in range(size)]
    return jnp.stack(blocks)


def total_of(value, axes):
    for axis in axes:
        for bit in axis_bits(axis):
            value = value + swap(value, axis, bit)
    return value


def merge_softmax(first, second):
    larger = jnp.maximum(first[0], second[0])
    total = first[1] * jnp.exp(first[0] - larger) + second[1] * jnp.exp(second[0] - larger)
    return jnp.stack([larger, total])


def body(
    tokens,
    expert_index,
    slot_index,
    norm_gain,
    router_weight,
    gate_weight,
    up_weight,
    down_weight,
    final_gain,
    head_weight,
):
    expert_devices = lax.axis_size("expert")
    model_devices = lax.axis_size("mp")
    token_devices = lax.axis_size("dp")
    local_tokens, local_features = tokens.shape
    expert_count = router_weight.shape[0]
    capacity = 3 * local_tokens // expert_count
    model_width = local_features * expert_devices * model_devices

    mp_bits = [("mp", bit) for bit in reversed(axis_bits("mp"))]
    dp_bits = [("dp", bit) for bit in reversed(axis_bits("dp"))]
    wide, last = mp_bits[:-1], mp_bits[-1:]
    paths = (wide + dp_bits + last, dp_bits + wide + last)
    half = expert_devices // 2

    flat_index = expert_index * capacity + slot_index
    every_slot = jnp.arange(expert_count * capacity, dtype=jnp.int32)
    chooser = jnp.any(flat_index[None, :, :] == every_slot[:, None, None], axis=2).astype(
        jnp.bfloat16
    )
    local_slots = jnp.dot(chooser, tokens, preferred_element_type=jnp.float32).astype(jnp.bfloat16)
    local_slots = local_slots.reshape(expert_count, capacity, local_features)
    gain_first = lax.reduce_precision(norm_gain, 8, 7)
    gain_second = lax.reduce_precision(norm_gain - gain_first, 8, 7)
    gain_third = norm_gain - gain_first - gain_second
    gain_part = jnp.stack([gain_first, gain_second, gain_third]).astype(jnp.bfloat16)
    gain_part = jnp.pad(gain_part, ((0, GAIN_ROWS - 3), (0, 0)))
    gain_part = jnp.broadcast_to(gain_part[None], (expert_count, GAIN_ROWS, local_features))
    sent = jnp.concatenate([local_slots, gain_part], axis=1)
    arrived = lax.all_to_all(sent, "expert", split_axis=0, concat_axis=0, tiled=True)

    tokens_float = tokens.astype(jnp.float32)
    gained = tokens_float * norm_gain[None, :]
    router_part = lax.dot_general(
        router_weight.astype(jnp.float32),
        gained,
        (((1,), (1,)), ((), ())),
        precision=lax.Precision.HIGHEST,
    )
    square_part = jnp.sum(tokens_float * tokens_float, axis=1)
    sums = total_of(jnp.concatenate([router_part, square_part[None]], axis=0), ("mp", "expert"))
    inverse = lax.rsqrt(sums[expert_count] / model_width + epsilon)
    router_logits = sums[:expert_count] * inverse[None, :]
    router_logsum = jax.nn.logsumexp(router_logits, axis=0)
    index_rows = expert_index.T
    expert_ids = jnp.arange(expert_count, dtype=jnp.int32)
    picked = jnp.sum(
        jnp.where(index_rows[:, None, :] == expert_ids[None, :, None], router_logits[None], 0.0),
        axis=1,
    )
    gate_weights = jax.nn.softmax(picked, axis=0)

    halves = [
        doubling(arrived[:half], paths[0]),
        doubling(arrived[half:], paths[1]),
    ]

    def block(d, m, e):
        side = 0 if e < half else 1
        got = piece_of(halves[side], paths[side], {"dp": d, "mp": m})
        return got[e - side * half]

    order = [(e, m) for e in range(expert_devices) for m in range(model_devices)]
    raw_rows = jnp.concatenate(
        [
            jnp.concatenate([block(d, m, e)[:capacity] for e, m in order], axis=1)
            for d in range(token_devices)
        ],
        axis=0,
    )
    gain_rows = jnp.concatenate([block(0, m, e)[capacity : capacity + 3] for e, m in order], axis=1)
    gain = jnp.sum(gain_rows.astype(jnp.float32), axis=0)
    raw_float = raw_rows.astype(jnp.float32)
    row_inverse = lax.rsqrt(jnp.mean(raw_float * raw_float, axis=1) + epsilon)
    row_piece = (raw_float * row_inverse[:, None] * gain[None, :]).astype(jnp.bfloat16)

    gate_value = lax.dot_general(
        row_piece, gate_weight[0], (((1,), (1,)), ((), ())), preferred_element_type=jnp.float32
    )
    up_value = lax.dot_general(
        row_piece, up_weight[0], (((1,), (1,)), ((), ())), preferred_element_type=jnp.float32
    )
    hidden = (jax.nn.silu(gate_value) * up_value).astype(jnp.bfloat16)
    partial = jnp.dot(hidden, down_weight[0], preferred_element_type=jnp.float32).astype(
        jnp.bfloat16
    )

    def partial_block(d, m, e):
        column = (e * model_devices + m) * local_features
        return partial[d * capacity : (d + 1) * capacity, column : column + local_features]

    def stacked(experts):
        blocks = [
            jnp.stack([partial_block(d, m, e) for e in experts])
            for m in range(model_devices)
            for d in range(token_devices)
        ]
        shape = (2,) * (len(mp_bits) + len(dp_bits)) + blocks[0].shape
        return jnp.stack(blocks).reshape(shape)

    dims = mp_bits + dp_bits
    summed = jnp.concatenate(
        [
            halving(stacked(range(half)), dims, last + wide + dp_bits),
            halving(stacked(range(half, expert_devices)), dims, last + dp_bits + wide),
        ],
        axis=0,
    )
    returned = lax.all_to_all(summed, "expert", split_axis=0, concat_axis=0, tiled=True)
    flat_out = returned.reshape(expert_count * capacity, local_features)
    combined = jnp.zeros((local_tokens, local_features), jnp.float32)
    for k in range(expert_index.shape[1]):
        selector = (flat_index[:, k][:, None] == every_slot[None, :]).astype(jnp.bfloat16)
        rows = jnp.dot(selector, flat_out, preferred_element_type=jnp.float32)
        combined = combined + gate_weights[k][:, None] * rows
    layer_out = (tokens_float + combined).astype(jnp.bfloat16)

    head_pieces = doubling(gather_direct(layer_out, "expert"), mp_bits)
    head_rows = jnp.concatenate(
        [piece_of(head_pieces, mp_bits, {"mp": m})[e] for e, m in order], axis=1
    )
    head_float = head_rows.astype(jnp.float32)
    head_scale = lax.rsqrt(jnp.mean(head_float * head_float, axis=1) + epsilon)
    head_in = (head_float * head_scale[:, None] * final_gain[None, :]).astype(jnp.bfloat16)
    logits = lax.dot_general(
        head_in, head_weight, (((1,), (1,)), ((), ())), preferred_element_type=jnp.float32
    )
    vocab_max = jnp.max(logits, axis=1)
    vocab_total = jnp.sum(jnp.exp(logits - vocab_max[:, None]), axis=1)
    pair = jnp.stack([vocab_max, vocab_total])
    for axis in ("mp", "expert"):
        for bit in axis_bits(axis):
            pair = merge_softmax(pair, swap(pair, axis, bit))
    head_logsum = pair[0] + jnp.log(pair[1])
    squares = jnp.stack(
        [jnp.sum(router_logsum * router_logsum), jnp.sum(head_logsum * head_logsum)]
    )
    means = total_of(squares, ("dp",)) / (local_tokens * token_devices)
    return (layer_out, head_logsum, means[0], means[1])


def solution(mesh):
    in_specs = (
        P("dp", ("expert", "mp")),
        P("dp", None),
        P("dp", None),
        P(("expert", "mp")),
        P(None, ("expert", "mp")),
        P("expert", ("dp", "mp"), None),
        P("expert", ("dp", "mp"), None),
        P("expert", ("dp", "mp"), None),
        P(),
        P(("expert", "mp"), None),
    )
    out_specs = (P("dp", ("expert", "mp")), P("dp"), P(), P())
    return jax.shard_map(body, mesh=mesh, in_specs=in_specs, out_specs=out_specs, check_vma=False)
```

```python
import jax
import jax.numpy as jnp
from jax import lax
from jax.sharding import PartitionSpec as P

epsilon = 1e-05
GAIN_ROWS = 16


def axis_bits(axis):
    size = lax.axis_size(axis)
    bits = []
    bit = 1
    while bit < size:
        bits.append(bit)
        bit *= 2
    return bits


def swap(value, axis, mask):
    size = lax.axis_size(axis)
    return lax.ppermute(value, axis, [(i, i ^ mask) for i in range(size)])


def upper(axis, bit):
    return (lax.axis_index(axis) & bit) != 0


def doubling(value, stages):
    for axis, bit in stages:
        other = swap(value, axis, bit)
        high = upper(axis, bit)
        value = jnp.stack([jnp.where(high, other, value), jnp.where(high, value, other)])
    return value


def piece_of(value, stages, place):
    index = tuple(1 if place[axis] & bit else 0 for axis, bit in reversed(stages))
    return value[index]


def halve(value, dims, stage):
    axis, bit = stage
    at = dims.index(stage)
    low = lax.index_in_dim(value, 0, at, keepdims=False)
    top = lax.index_in_dim(value, 1, at, keepdims=False)
    high = upper(axis, bit)
    arrived = swap(jnp.where(high, low, top), axis, bit)
    kept = jnp.where(high, top, low)
    value = (kept.astype(jnp.float32) + arrived.astype(jnp.float32)).astype(value.dtype)
    return value, [other for other in dims if other != stage]


def gather_direct(value, axis):
    size = lax.axis_size(axis)
    blocks = [value] + [swap(value, axis, mask) for mask in range(1, size)]
    for bit in axis_bits(axis):
        high = upper(axis, bit)
        blocks = [jnp.where(high, blocks[k ^ bit], blocks[k]) for k in range(size)]
    return jnp.stack(blocks)


def total_of(value, stages):
    for axis, bit in stages:
        value = value + swap(value, axis, bit)
    return value


def merge_over(value, axis):
    size = lax.axis_size(axis)
    parts = jnp.stack([value] + [swap(value, axis, mask) for mask in range(1, size)])
    largest = jnp.max(parts[:, :, 0], axis=0)
    scaled = parts[:, :, 1] * jnp.exp(parts[:, :, 0] - largest[None])
    while scaled.shape[0] > 1:
        scaled = scaled[0::2] + scaled[1::2]
    return jnp.stack([largest, scaled[0]], axis=1)


def body(
    tokens,
    expert_index,
    slot_index,
    norm_gain,
    router_weight,
    gate_weight,
    up_weight,
    down_weight,
    final_gain,
    head_weight,
):
    expert_devices = lax.axis_size("expert")
    model_devices = lax.axis_size("mp")
    token_devices = lax.axis_size("dp")
    local_tokens, local_features = tokens.shape
    expert_count = router_weight.shape[0]
    capacity = 3 * local_tokens // expert_count
    model_width = local_features * expert_devices * model_devices

    mp_bits = [("mp", bit) for bit in reversed(axis_bits("mp"))]
    dp_bits = [("dp", bit) for bit in reversed(axis_bits("dp"))]
    wide, last = mp_bits[:-1], mp_bits[-1:]
    paths = (wide + dp_bits + last, dp_bits + wide + last)
    half = expert_devices // 2

    flat_index = expert_index * capacity + slot_index
    every_slot = jnp.arange(expert_count * capacity, dtype=jnp.int32)
    chooser = jnp.any(flat_index[None, :, :] == every_slot[:, None, None], axis=2).astype(
        jnp.bfloat16
    )
    local_slots = jnp.dot(chooser, tokens, preferred_element_type=jnp.float32).astype(jnp.bfloat16)
    local_slots = local_slots.reshape(expert_count, capacity, local_features)
    gain_first = lax.reduce_precision(norm_gain, 8, 7)
    gain_second = lax.reduce_precision(norm_gain - gain_first, 8, 7)
    gain_third = norm_gain - gain_first - gain_second
    gain_part = jnp.stack([gain_first, gain_second, gain_third]).astype(jnp.bfloat16)
    gain_part = jnp.pad(gain_part, ((0, GAIN_ROWS - 3), (0, 0)))
    gain_part = jnp.broadcast_to(gain_part[None], (expert_count, GAIN_ROWS, local_features))
    sent = jnp.concatenate([local_slots, gain_part], axis=1)
    arrived = lax.all_to_all(sent, "expert", split_axis=0, concat_axis=0, tiled=True)

    tokens_float = tokens.astype(jnp.float32)
    gained = tokens_float * norm_gain[None, :]
    router_part = lax.dot_general(
        router_weight.astype(jnp.float32),
        gained,
        (((1,), (1,)), ((), ())),
        precision=lax.Precision.HIGHEST,
    )
    square_part = jnp.sum(tokens_float * tokens_float, axis=1)
    router_sums = jnp.concatenate([router_part, square_part[None]], axis=0)

    halves = [
        doubling(arrived[:half], paths[0]),
        doubling(arrived[half:], paths[1]),
    ]

    def block(d, m, e):
        side = 0 if e < half else 1
        got = piece_of(halves[side], paths[side], {"dp": d, "mp": m})
        return got[e - side * half]

    order = [(e, m) for e in range(expert_devices) for m in range(model_devices)]
    raw_rows = jnp.concatenate(
        [
            jnp.concatenate([block(d, m, e)[:capacity] for e, m in order], axis=1)
            for d in range(token_devices)
        ],
        axis=0,
    )
    gain_rows = jnp.concatenate([block(0, m, e)[capacity : capacity + 3] for e, m in order], axis=1)
    gain = jnp.sum(gain_rows.astype(jnp.float32), axis=0)
    raw_float = raw_rows.astype(jnp.float32)
    row_inverse = lax.rsqrt(jnp.mean(raw_float * raw_float, axis=1) + epsilon)
    row_piece = (raw_float * row_inverse[:, None] * gain[None, :]).astype(jnp.bfloat16)

    gate_value = lax.dot_general(
        row_piece, gate_weight[0], (((1,), (1,)), ((), ())), preferred_element_type=jnp.float32
    )
    up_value = lax.dot_general(
        row_piece, up_weight[0], (((1,), (1,)), ((), ())), preferred_element_type=jnp.float32
    )
    hidden = (jax.nn.silu(gate_value) * up_value).astype(jnp.bfloat16)
    partial = jnp.dot(hidden, down_weight[0], preferred_element_type=jnp.float32).astype(
        jnp.bfloat16
    )

    def partial_block(d, m, e):
        column = (e * model_devices + m) * local_features
        return partial[d * capacity : (d + 1) * capacity, column : column + local_features]

    def stacked(experts):
        blocks = [
            jnp.stack([partial_block(d, m, e) for e in experts])
            for m in range(model_devices)
            for d in range(token_devices)
        ]
        shape = (2,) * (len(mp_bits) + len(dp_bits)) + blocks[0].shape
        return jnp.stack(blocks).reshape(shape)

    router_stages = [(axis, bit) for axis in ("mp", "expert") for bit in axis_bits(axis)]
    back = (last + wide + dp_bits, last + dp_bits + wide)
    dims = [mp_bits + dp_bits, mp_bits + dp_bits]
    sums = [stacked(range(half)), stacked(range(half, expert_devices))]
    for step in range(len(back[0])):
        sums[0], sums[1], router_sums = lax.optimization_barrier((sums[0], sums[1], router_sums))
        for side in range(2):
            sums[side], dims[side] = halve(sums[side], dims[side], back[side][step])
        router_sums = total_of(router_sums, router_stages[step : step + 1])
    summed = jnp.concatenate(sums, axis=0)
    summed, router_sums = lax.optimization_barrier((summed, router_sums))
    router_sums = total_of(router_sums, router_stages[len(back[0]) :])
    inverse = lax.rsqrt(router_sums[expert_count] / model_width + epsilon)
    router_logits = router_sums[:expert_count] * inverse[None, :]
    router_logsum = jax.nn.logsumexp(router_logits, axis=0)
    index_rows = expert_index.T
    expert_ids = jnp.arange(expert_count, dtype=jnp.int32)
    picked = jnp.sum(
        jnp.where(index_rows[:, None, :] == expert_ids[None, :, None], router_logits[None], 0.0),
        axis=1,
    )
    gate_weights = jax.nn.softmax(picked, axis=0)
    returned = lax.all_to_all(summed, "expert", split_axis=0, concat_axis=0, tiled=True)
    flat_out = returned.reshape(expert_count * capacity, local_features)
    combined = jnp.zeros((local_tokens, local_features), jnp.float32)
    for k in range(expert_index.shape[1]):
        selector = (flat_index[:, k][:, None] == every_slot[None, :]).astype(jnp.bfloat16)
        rows = jnp.dot(selector, flat_out, preferred_element_type=jnp.float32)
        combined = combined + gate_weights[k][:, None] * rows
    layer_out = (tokens_float + combined).astype(jnp.bfloat16)

    cut = local_tokens * 11 // 16
    first_pieces = doubling(gather_direct(layer_out[:cut], "expert"), mp_bits)
    second_pieces = doubling(
        gather_direct(doubling(layer_out[cut:], wide), "expert"), last
    )

    def second_piece(m, e):
        return piece_of(piece_of(second_pieces, last, {"mp": m})[e], wide, {"mp": m})

    head_rows = jnp.concatenate(
        [
            jnp.concatenate([piece_of(first_pieces, mp_bits, {"mp": m})[e] for e, m in order], axis=1),
            jnp.concatenate([second_piece(m, e) for e, m in order], axis=1),
        ],
        axis=0,
    )
    head_float = head_rows.astype(jnp.float32)
    head_scale = lax.rsqrt(jnp.mean(head_float * head_float, axis=1) + epsilon)
    head_in = (head_float * head_scale[:, None] * final_gain[None, :]).astype(jnp.bfloat16)
    logits = lax.dot_general(
        head_in, head_weight, (((1,), (1,)), ((), ())), preferred_element_type=jnp.float32
    )
    vocab_max = jnp.max(logits, axis=1)
    vocab_total = jnp.sum(jnp.exp(logits - vocab_max[:, None]), axis=1)
    pair = jnp.stack([vocab_max, vocab_total])[None]
    for axis, bit in reversed(dp_bits):
        pair = jnp.concatenate([pair, swap(pair, axis, bit)])
    for axis in ("mp", "expert"):
        pair = merge_over(pair, axis)
    logsums = pair[:, 0] + jnp.log(pair[:, 1])
    head_squares = jnp.sum(logsums * logsums, axis=1)
    while head_squares.shape[0] > 1:
        head_squares = head_squares[0::2] + head_squares[1::2]
    router_square = total_of(jnp.sum(router_logsum * router_logsum, keepdims=True), dp_bits)
    token_total = local_tokens * token_devices
    return (layer_out, logsums[0], router_square[0] / token_total, head_squares[0] / token_total)


def solution(mesh):
    in_specs = (
        P("dp", ("expert", "mp")),
        P("dp", None),
        P("dp", None),
        P(("expert", "mp")),
        P(None, ("expert", "mp")),
        P("expert", ("dp", "mp"), None),
        P("expert", ("dp", "mp"), None),
        P("expert", ("dp", "mp"), None),
        P(),
        P(("expert", "mp"), None),
    )
    out_specs = (P("dp", ("expert", "mp")), P("dp"), P(), P())
    return jax.shard_map(body, mesh=mesh, in_specs=in_specs, out_specs=out_specs, check_vma=False)
```
